256 devices in a mesh: rows: 64 (over z, x, y_lo), grp: 4 (over y_hi, core).
Axes of the slice: x: 4, y: 4 (y_hi: 2, y_lo: 2; y = y_hi * 2 + y_lo), z: 8, core: 2. Of those that a mesh axis runs over, the one named last changes fastest.
Arguments:
- visibilities: float32 [2, 1048576], P(None, ('rows', 'grp')), may hold values from -6 to 6
- uv_tiles: int32 [2, 1048576], P(None, ('rows', 'grp')), may hold values from 0 to 511, as said below
- kernel_offsets: int32 [2, 1048576], P(None, ('rows', 'grp')), may hold values from 0 to 7
- kernel: float32 [8, 8], replicated, may hold values from 0.5 to 1.5
Outputs:
- dirty_image: float32 [2, 4096, 4096], P(None, ('rows', 'grp'))
The draws below stay inside these ranges and needn't reach their ends.
Inputs may be any that keep to these rules, and one draw needn't show every extreme that they name: `uv_tiles`: row 0 holds tile rows, row 1 tile columns. The visibilities of baseline block q (positions q * 4096 to (q + 1) * 4096 - 1), with s = q divided by the number of devices of grp, have tile rows from s * 8 to (s + 1) * 8 - 1.
All inputs are finite; a program needn't handle non-finite values.
Results may differ from the reference program's by a relative error of at most 0.0044.
Values sent between devices are 32-bit elements; how exact they have to be, the bound alone decides.
A program may use at most 64 MiB of HBM per device.

```python
import jax
import jax.numpy as jnp
from jax import lax

G = 4096
TAPS = 8
VIS_DEV = 4096
VIS = 1048576
SLAB = 64
N_GRP = 4


def draw_uv_tiles(key, part):
    first_key, second_key = jax.random.split(jax.random.fold_in(key, 17))
    position = jnp.arange(VIS, dtype=jnp.int32)
    slab_index = position // (VIS_DEV * N_GRP)
    tiles_slab = SLAB // TAPS
    tile_rows = slab_index * tiles_slab + jax.random.randint(first_key, (VIS,), 0, tiles_slab, dtype=jnp.int32)
    tile_cols = jax.random.randint(second_key, (VIS,), 0, G // TAPS, dtype=jnp.int32)
    return jnp.stack([tile_rows, tile_cols]).astype(jnp.int32)


def plant(drawn, own_key, low, top_value):
    longest = drawn.shape.index(max(drawn.shape))
    spots = []
    for shift in (0, 1):
        where = [jax.random.randint(jax.random.fold_in(own_key, axis), (), 0, length) for axis, length in enumerate(drawn.shape)]
        where[longest] = (where[longest] + shift) % drawn.shape[longest]
        spots.append(tuple(where))
    return drawn.at[spots[0]].set(low).at[spots[1]].set(top_value)


def level_of(own_key, extent, cuts, low, top_value):
    gain, own = 1.0, jax.random.fold_in(own_key, 6)
    for axis_at, blocks in cuts:
        heights = jnp.exp(jax.random.uniform(jax.random.fold_in(own, axis_at), (blocks,), jnp.float32, low / len(cuts), top_value / len(cuts)))
        gain = gain * jnp.repeat(heights, extent[axis_at] // blocks).reshape([-1 if axis == axis_at else 1 for axis in range(len(extent))])
    return gain


def noise(stream_key, extent, scale, limit, cuts=(), kind=jnp.bfloat16):
    values = scale * jax.random.normal(stream_key, extent, jnp.float32)
    if cuts:
        values = values * level_of(stream_key, extent, cuts, -0.22, 0.18)
    return jnp.clip(values, -limit, limit).astype(kind)


def setup_inputs(seed: int = 0) -> dict:
    splits = jax.random.split(jax.random.key(seed), 5)
    visibilities = noise(splits[0], (2, VIS), 1.0, 6.0, ((1, 256),), jnp.float32)
    uv_tiles = draw_uv_tiles(jax.random.fold_in(splits[4], 71), 0)
    kernel_offsets = plant(jax.random.randint(splits[2], (2, VIS), 0, TAPS), jax.random.fold_in(splits[2], 1), 0, TAPS - 1).astype(jnp.int32)
    kernel = jnp.clip(jax.random.uniform(splits[3], (TAPS, TAPS), jnp.float32, 0.5, 1.5), 0.5, 1.5)
    return {"visibilities": visibilities, "uv_tiles": uv_tiles, "kernel_offsets": kernel_offsets, "kernel": kernel}


def reference(visibilities, uv_tiles, kernel_offsets, kernel):
    tap_count = kernel.shape[0]
    row_start = tap_count * uv_tiles[0] + kernel_offsets[0]
    col_start = tap_count * uv_tiles[1] + kernel_offsets[1]
    row_taps = lax.optimization_barrier(kernel[kernel_offsets[0]].astype(jnp.bfloat16)).astype(jnp.float32)
    col_taps = kernel[kernel_offsets[1]]
    col_real = lax.optimization_barrier((visibilities[0][:, None] * col_taps).astype(jnp.bfloat16)).astype(jnp.float32)
    col_imag = lax.optimization_barrier((visibilities[1][:, None] * col_taps).astype(jnp.bfloat16)).astype(jnp.float32)
    col_index = (col_start[:, None] + jnp.arange(tap_count, dtype=jnp.int32)[None, :]) % G
    grid_real = jnp.zeros((G, G), jnp.float32)
    grid_imag = jnp.zeros((G, G), jnp.float32)
    for tap_index in range(tap_count):
        row_index = ((row_start + tap_index) % G)[:, None]
        weight = row_taps[:, tap_index:tap_index + 1]
        grid_real = grid_real.at[row_index, col_index].add(weight * col_real)
        grid_imag = grid_imag.at[row_index, col_index].add(weight * col_imag)
    spectrum = jnp.fft.ifft2(grid_real + 1j * grid_imag) * G
    return jnp.stack([jnp.real(spectrum).T, jnp.imag(spectrum).T]).astype(jnp.float32)
```

```python
import functools

import jax
import jax.numpy as jnp
import numpy as np
from jax import lax
from jax.experimental import pallas as pl
from jax.experimental.pallas import tpu as pltpu
from jax.sharding import PartitionSpec as P

G = 4096
MESH = pl.DeviceIdType.MESH
BF16 = jnp.bfloat16
F32 = jnp.float32
CHUNK = 512
N_VIS = 4096
ROWS_W = 272
ROWS_S = 48


def split_table(x):
    hi = x.astype(np.float32).astype(jnp.dtype(BF16))
    return hi, (x - hi.astype(np.float64)).astype(np.float32).astype(jnp.dtype(BF16))


def unit(turns):
    angle = 2.0 * np.pi * (turns % 1.0)
    return np.cos(angle), np.sin(angle)


@functools.cache
def tables_v():
    h = np.arange(16)
    er, ei = unit(h[:, None] * h[None, :] / 16)
    d = np.concatenate([np.kron(np.eye(16), er), np.kron(np.eye(16), ei)], axis=1)
    w, lane = np.arange(ROWS_W), np.arange(128)
    tr, ti = unit(w[:, None] * (lane % 16)[None, :] / 4096)
    tw = np.stack([tr, ti]).astype(np.float32) / np.float32(G)
    q = np.arange(256)
    wr, wi = unit(q[:, None] * q[None, :] / 256)
    big = np.block([[wr, -wi], [wi, wr]])
    return split_table(d) + (tw,) + split_table(big)


@functools.cache
def tables_u():
    k, s = np.arange(128), np.arange(64)
    er, ei = unit(k[:, None] * s[None, :] / 64)
    e = np.block([[er, -ei], [ei, er]])
    lane = np.arange(128)
    tr, ti = unit(k[:, None] * (lane // 16)[None, :] / 512)
    tw1 = np.stack([tr, ti]).astype(np.float32)
    row = np.arange(64)
    dr, di = unit((row // 16)[:, None] * (lane // 16)[None, :] / 4)
    same = (row % 16)[:, None] == (lane % 16)[None, :]
    d = np.concatenate([dr * same, di * same], axis=0)
    j, k1 = np.arange(8), np.arange(4)
    ar, ai = unit(j[:, None, None] * (k[None, None, :] + 128 * k1[None, :, None]) / 4096)
    tw2 = np.stack([ar.reshape(32, 128), ai.reshape(32, 128)]).astype(np.float32)
    return split_table(e) + (tw1,) + split_table(d) + (tw2,)


def halves(x):
    hi = x.astype(BF16)
    return hi, (x - hi.astype(F32)).astype(BF16)


def dot(a, b, dims):
    return lax.dot_general(a, b, (dims, ((), ())), preferred_element_type=F32)


def dot3(a, b, dims):
    return dot(a[0], b[0], dims) + (dot(a[1], b[0], dims) + dot(a[0], b[1], dims))


NN = ((1,), (0,))
NT = ((1,), (1,))


def build_tables(kern_ref, g, tab_ref):
    sub = lax.broadcasted_iota(jnp.int32, (8, 128), 0)
    for o in range(8):
        col = jnp.zeros((8, 128), F32)
        row = jnp.zeros((8, 128), F32)
        for j in range(8):
            col = jnp.where(sub == j, kern_ref[o, (j - o) % 8], col)
            row = jnp.where(sub == j, kern_ref[o, lax.rem(g + (j - o) % 8, 8)], row)
        tab_ref[o] = col
        tab_ref[8 + o] = row.astype(BF16).astype(F32)


def pick(which, tab_ref, first):
    out = jnp.zeros((8, 128), F32)
    for o in range(8):
        out = jnp.where(which == o, tab_ref[first + o], out)
    return out


def build(vis_ref, tile_ref, off_ref, start, slab, g, tab_ref, parts):
    bt, at, sa, sb = parts
    sub8 = lax.broadcasted_iota(jnp.int32, (8, 128), 0)
    sub16 = lax.broadcasted_iota(jnp.int32, (16, 128), 0)
    half = sub16 // 8
    zero = jnp.zeros((16, 128), BF16)

    def wide(x, rows):
        return jnp.broadcast_to(x, (rows, 128))

    def as_bf16(x):
        return x.astype(F32).astype(BF16)

    for q in range(CHUNK // 128):
        here = pl.ds(start + q * 128, 128)
        lanes = slice(q * 128, (q + 1) * 128)
        tile_row = tile_ref[0:1, here] - 8 * slab
        tile_col = tile_ref[1:2, here]
        off_row = off_ref[0:1, here]
        off_col = off_ref[1:2, here]
        if bt is not None or sb is not None:
            taps = pick(wide(off_col, 8), tab_ref, 0)
            wrapped = (sub8 < off_col).astype(jnp.int32)
            carry = jnp.concatenate([wrapped, wrapped], axis=0) - half
            values = []
            for c in range(2):
                one = vis_ref[c : c + 1, here] * taps
                values.append(jnp.concatenate([one, one], axis=0).astype(BF16))
        if bt is not None:
            need = as_bf16(carry + (tile_col & 31))
            for m in range(17):
                hit = need == BF16(2 * m)
                for c in range(2):
                    bt[c * ROWS_W + 16 * m : c * ROWS_W + 16 * m + 16, lanes] = jnp.where(hit, values[c], zero)
        if sb is not None:
            need = as_bf16(carry + (tile_col & 3))
            for m in range(3):
                hit = need == BF16(2 * m)
                for c in range(2):
                    sb[c * ROWS_S + 16 * m : c * ROWS_S + 16 * m + 16, lanes] = jnp.where(hit, values[c], zero)
        if at is not None or sa is not None:
            row_taps = pick(wide(off_row, 8), tab_ref, 8)
            own_h = sub16 == wide(tile_col >> 5, 16)
            fine = (tile_col >> 2) & 7
            for b in range(2):
                spread = jnp.where(own_h, wide(row_taps[4 * b : 4 * b + 1], 16), 0.0).astype(BF16)
                row_tile = tile_row + (4 * b + g < off_row).astype(jnp.int32)
                if at is not None:
                    need = as_bf16(wide(row_tile, 16))
                    for t in range(8):
                        first = b * 128 + t * 16
                        at[first : first + 16, lanes] = jnp.where(need == BF16(t), spread, zero)
                if sa is not None:
                    need = as_bf16(wide(jnp.where(row_tile == 8, fine, -1), 16))
                    for t in range(8):
                        first = b * 128 + t * 16
                        sa[first : first + 16, lanes] = jnp.where(need == BF16(t), spread, zero)


def grid_block(vis_ref, tile_ref, off_ref, slab, g, tab_ref, scratch, main, spill):
    bt, at, sa, sb, acc, accs = scratch

    def step(i, _):
        start = pl.multiple_of(i * CHUNK, CHUNK)
        parts = (bt if main else None, at if main else None, sa if spill else None, sb if spill else None)
        build(vis_ref, tile_ref, off_ref, start, slab, g, tab_ref, parts)
        if main:
            acc[...] += dot(bt[...], at[...], NT)
        if spill:
            accs[...] += dot(sa[...], sb[...], NT)
        return 0

    lax.fori_loop(0, N_VIS // CHUNK, step, 0)


def add_spill(acc, got):
    for c in range(2):
        for b in range(2):
            for f in range(8):
                rows = pl.ds(c * ROWS_W + 32 * f, ROWS_S)
                acc[rows, b * 128 : b * 128 + 16] += got[
                    c * ROWS_S : (c + 1) * ROWS_S, b * 128 + f * 16 : b * 128 + f * 16 + 16
                ]


def row_transform(acc, d_hi, d_lo, tw, w_hi, w_lo, out_ref):
    n = ROWS_W
    p = dot3(halves(acc[...]), (d_hi[...], d_lo[...]), NN)
    real = p[:n, :256] - p[n:, 256:]
    imag = p[:n, 256:] + p[n:, :256]
    cos = jnp.concatenate([tw[0], tw[0]], axis=1)
    sin = jnp.concatenate([tw[1], tw[1]], axis=1)
    turned = (real * cos - imag * sin, real * sin + imag * cos)
    both = jnp.concatenate([jnp.concatenate([t[:16] + t[256:], t[16:256]], axis=0) for t in turned], axis=0)
    s = dot3((w_hi[...], w_lo[...]), halves(both), NN)
    for c in range(2):
        for b in range(2):
            out_ref[pl.ds(2 * c + b, 256, stride=4), :] = s[c * 256 : (c + 1) * 256, b * 128 : (b + 1) * 128]


def grid_kernel(
    vis, tiles, offs, kern, d_hi, d_lo, tw, w_hi, w_lo, out_ref,
    got_vis, got_tiles, got_offs, tab, bt, at, sa, sb, acc, accs, spill_out, spill_in,
    send_sems, recv_sems, spill_sems,
):
    slab, g = lax.axis_index("rows"), lax.axis_index("grp")
    slabs = lax.axis_size("rows")
    after, before = lax.rem(slab + 1, slabs), lax.rem(slab + slabs - 1, slabs)
    low = lax.rem(g, 2)
    sibling = g + 1 - 2 * low
    across = lax.rem(g + 2, 4)

    barrier = pltpu.get_barrier_semaphore()
    for peer in ((slab, sibling), (slab, across), (after, g), (before, g)):
        pl.semaphore_signal(barrier, inc=1, device_id=peer, device_id_type=MESH)

    build_tables(kern, g, tab)
    acc[...] = jnp.zeros_like(acc)
    accs[...] = jnp.zeros_like(accs)
    pl.semaphore_wait(barrier, 4)

    def send(sources, slot, peer):
        copies = []
        for n, (source, target) in enumerate(zip(sources, (got_vis, got_tiles, got_offs))):
            copies.append(
                pltpu.make_async_remote_copy(
                    src_ref=source,
                    dst_ref=target.at[slot],
                    send_sem=send_sems.at[slot, n],
                    recv_sem=recv_sems.at[slot, n],
                    device_id=(slab, peer),
                    device_id_type=MESH,
                )
            )
        for copy in copies:
            copy.start()
        return copies

    own = (vis, tiles, offs)
    held = [own] + [(got_vis.at[n], got_tiles.at[n], got_offs.at[n]) for n in range(3)]
    to_across = send(own, 1, across)
    to_sibling = send(own, 0, sibling)
    scratch = (bt, at, sa, sb, acc, accs)

    def block(n, main, spill):
        grid_block(*held[n], slab, g, tab, scratch, main, spill)

    block(0, True, True)
    for copy in to_sibling:
        copy.wait_recv()
    block(1, True, True)
    for copy in to_across:
        copy.wait_recv()
    relayed = send(held[2], 2, sibling)
    block(2, False, True)
    for copy in relayed:
        copy.wait_recv()
    block(3, False, True)
    spill_out[...] = accs[...].T
    spill_copy = pltpu.make_async_remote_copy(
        src_ref=spill_out,
        dst_ref=spill_in,
        send_sem=spill_sems.at[0],
        recv_sem=spill_sems.at[1],
        device_id=(after, g),
        device_id_type=MESH,
    )
    spill_copy.start()
    block(2, True, False)
    block(3, True, False)
    spill_copy.wait_recv()
    add_spill(acc, spill_in)
    row_transform(acc, d_hi, d_lo, tw, w_hi, w_lo, out_ref)
    for copy in to_sibling + to_across + relayed + [spill_copy]:
        copy.wait_send()


def vmem(shape, dtype):
    return pltpu.VMEM(shape, dtype)


def grid_scratch():
    return [
        vmem((16, 8, 128), F32),
        vmem((2 * ROWS_W, CHUNK), BF16),
        vmem((256, CHUNK), BF16),
        vmem((256, CHUNK), BF16),
        vmem((2 * ROWS_S, CHUNK), BF16),
        vmem((2 * ROWS_W, 256), F32),
        vmem((256, 2 * ROWS_S), F32),
        vmem((2 * ROWS_S, 256), F32),
        vmem((2 * ROWS_S, 256), F32),
    ]


def row_stage(visibilities, uv_tiles, kernel_offsets, kernel):
    in_vmem = pl.BlockSpec(memory_space=pltpu.VMEM)
    return pl.pallas_call(
        grid_kernel,
        out_shape=jax.ShapeDtypeStruct((1024, 128), F32),
        in_specs=[in_vmem] * 3 + [pl.BlockSpec(memory_space=pltpu.SMEM)] + [in_vmem] * 5,
        out_specs=in_vmem,
        scratch_shapes=[
            vmem((3, 2, N_VIS), F32),
            vmem((3, 2, N_VIS), jnp.int32),
            vmem((3, 2, N_VIS), jnp.int32),
        ]
        + grid_scratch()
        + [
            pltpu.SemaphoreType.DMA((3, 3)),
            pltpu.SemaphoreType.DMA((3, 3)),
            pltpu.SemaphoreType.DMA((2,)),
        ],
        compiler_params=pltpu.CompilerParams(
            collective_id=0, has_side_effects=True, vmem_limit_bytes=50 * 2**20
        ),
        name="grid_rows",
    )(visibilities, uv_tiles, kernel_offsets, kernel, *tables_v())


def fft8(x):
    def add(a, b):
        return (a[0] + b[0], a[1] + b[1])

    def sub(a, b):
        return (a[0] - b[0], a[1] - b[1])

    def by_i(a):
        return (-a[1], a[0])

    def fft4(a):
        s, d = add(a[0], a[2]), sub(a[0], a[2])
        t, e = add(a[1], a[3]), by_i(sub(a[1], a[3]))
        return [add(s, t), add(d, e), sub(s, t), sub(d, e)]

    root = np.float32(np.sqrt(0.5))
    even, odd = fft4(x[0::2]), fft4(x[1::2])
    one, three = odd[1], odd[3]
    odd[1] = (root * (one[0] - one[1]), root * (one[0] + one[1]))
    odd[2] = by_i(odd[2])
    odd[3] = (root * (-three[0] - three[1]), root * (three[0] - three[1]))
    return [add(even[k], odd[k]) for k in range(4)] + [sub(even[k], odd[k]) for k in range(4)]


def column_kernel(r_ref, e_hi, e_lo, tw1, d_hi, d_lo, tw2, out_ref):
    sums = []
    for j in range(8):
        b, g = divmod(j, 4)
        x = jnp.concatenate([r_ref[pl.ds(4 * g + 2 * c + b, 64, stride=16), :] for c in range(2)], axis=0)
        z = dot3((e_hi[...], e_lo[...]), halves(x), NN)
        real, imag = z[:128], z[128:]
        cos, sin = tw1[0], tw1[1]
        turned = jnp.concatenate([real * cos - imag * sin, real * sin + imag * cos], axis=0)
        p = dot3((d_hi[...], d_lo[...]), halves(turned), NT)
        real = p[:64, :128] - p[64:, 128:]
        imag = p[:64, 128:] + p[64:, :128]
        cos = jnp.concatenate([jnp.broadcast_to(tw2[0, 4 * j + k : 4 * j + k + 1], (16, 128)) for k in range(4)], axis=0)
        sin = jnp.concatenate([jnp.broadcast_to(tw2[1, 4 * j + k : 4 * j + k + 1], (16, 128)) for k in range(4)], axis=0)
        sums.append((real * cos - imag * sin, real * sin + imag * cos))
    for k2, pair in enumerate(fft8(sums)):
        for c in range(2):
            for k1 in range(4):
                first = 512 * k2 + 128 * k1
                out_ref[c, :, first : first + 128] = pair[c][16 * k1 : 16 * k1 + 16]


def column_stage(received):
    return pl.pallas_call(
        column_kernel,
        out_shape=jax.ShapeDtypeStruct((2, 16, G), F32),
        in_specs=[pl.BlockSpec(memory_space=pltpu.VMEM)] * 7,
        out_specs=pl.BlockSpec(memory_space=pltpu.VMEM),
        compiler_params=pltpu.CompilerParams(vmem_limit_bytes=40 * 2**20),
        name="columns",
    )(received, *tables_u())


def shards(visibilities, uv_tiles, kernel_offsets, kernel):
    blocks = row_stage(visibilities, uv_tiles, kernel_offsets, kernel)
    received = lax.all_to_all(
        blocks.reshape(256, 4, 128), ("rows", "grp"), split_axis=0, concat_axis=0, tiled=True
    )
    return column_stage(received.reshape(1024, 128))


def solution(mesh):
    in_specs = (P(None, ("rows", "grp")), P(None, ("rows", "grp")), P(None, ("rows", "grp")), P())
    out_specs = P(None, ("rows", "grp"), None)
    return jax.shard_map(shards, mesh=mesh, in_specs=in_specs, out_specs=out_specs, check_vma=False)
```

```python
import functools

import jax
import jax.numpy as jnp
import numpy as np
from jax import lax
from jax.experimental import pallas as pl
from jax.experimental.pallas import tpu as pltpu
from jax.sharding import PartitionSpec as P

G = 4096
MESH = pl.DeviceIdType.MESH
BF16 = jnp.bfloat16
F32 = jnp.float32
CHUNK = 1024
N_VIS = 4096
ROWS_W = 272
ROWS_S = 48


def split_table(x):
    hi = x.astype(np.float32).astype(jnp.dtype(BF16))
    return hi, (x - hi.astype(np.float64)).astype(np.float32).astype(jnp.dtype(BF16))


def unit(turns):
    angle = 2.0 * np.pi * (turns % 1.0)
    return np.cos(angle), np.sin(angle)


@functools.cache
def tables_v():
    h = np.arange(16)
    er, ei = unit(h[:, None] * h[None, :] / 16)
    d = np.concatenate([np.kron(np.eye(16), er), np.kron(np.eye(16), ei)], axis=1)
    w, lane = np.arange(ROWS_W), np.arange(128)
    tr, ti = unit(w[:, None] * (lane % 16)[None, :] / 4096)
    tw = np.stack([tr, ti]).astype(np.float32) / np.float32(G)
    q = np.arange(256)
    wr, wi = unit(q[:, None] * q[None, :] / 256)
    big = np.block([[wr, -wi], [wi, wr]])
    return split_table(d) + (tw,) + split_table(big)


@functools.cache
def tables_u():
    k, s = np.arange(128), np.arange(64)
    er, ei = unit(k[:, None] * s[None, :] / 64)
    e = np.block([[er, -ei], [ei, er]])
    lane = np.arange(128)
    tr, ti = unit(k[:, None] * (lane // 16)[None, :] / 512)
    tw1 = np.stack([tr, ti]).astype(np.float32)
    row = np.arange(64)
    dr, di = unit((row // 16)[:, None] * (lane // 16)[None, :] / 4)
    same = (row % 16)[:, None] == (lane % 16)[None, :]
    d = np.concatenate([dr * same, di * same], axis=0)
    j, k1 = np.arange(8), np.arange(4)
    ar, ai = unit(j[:, None, None] * (k[None, None, :] + 128 * k1[None, :, None]) / 4096)
    tw2 = np.stack([ar.reshape(32, 128), ai.reshape(32, 128)]).astype(np.float32)
    return split_table(e) + (tw1,) + split_table(d) + (tw2,)


def halves(x):
    hi = x.astype(BF16)
    return hi, (x - hi.astype(F32)).astype(BF16)


def dot(a, b, dims):
    return lax.dot_general(a, b, (dims, ((), ())), preferred_element_type=F32)


def dot3(a, b, dims):
    return dot(a[0], b[0], dims) + (dot(a[1], b[0], dims) + dot(a[0], b[1], dims))


NN = ((1,), (0,))
NT = ((1,), (1,))


def build_tables(kern_ref, g, tab_ref):
    sub = lax.broadcasted_iota(jnp.int32, (8, 128), 0)
    for o in range(8):
        col = jnp.zeros((8, 128), F32)
        row = jnp.zeros((8, 128), F32)
        for j in range(8):
            col = jnp.where(sub == j, kern_ref[o, (j - o) % 8], col)
            row = jnp.where(sub == j, kern_ref[o, lax.rem(g + (j - o) % 8, 8)], row)
        tab_ref[o] = col
        tab_ref[8 + o] = row.astype(BF16).astype(F32)


def pick(which, tab_ref, first):
    out = jnp.zeros((8, 128), F32)
    for o in range(8):
        out = jnp.where(which == o, tab_ref[first + o], out)
    return out


def build(vis_ref, tile_ref, off_ref, start, slab, g, tab_ref, parts):
    bt, at, sa, sb = parts
    sub8 = lax.broadcasted_iota(jnp.int32, (8, 128), 0)
    sub16 = lax.broadcasted_iota(jnp.int32, (16, 128), 0)
    half = sub16 // 8
    zero = jnp.zeros((16, 128), BF16)

    def wide(x, rows):
        return jnp.broadcast_to(x, (rows, 128))

    def as_bf16(x):
        return x.astype(F32).astype(BF16)

    for q in range(CHUNK // 128):
        here = pl.ds(start + q * 128, 128)
        lanes = slice(q * 128, (q + 1) * 128)
        tile_row = tile_ref[0:1, here] - 8 * slab
        tile_col = tile_ref[1:2, here]
        off_row = off_ref[0:1, here]
        off_col = off_ref[1:2, here]
        if bt is not None or sb is not None:
            taps = pick(wide(off_col, 8), tab_ref, 0)
            wrapped = (sub8 < off_col).astype(jnp.int32)
            carry = jnp.concatenate([wrapped, wrapped], axis=0) - half
            values = []
            for c in range(2):
                one = vis_ref[c : c + 1, here] * taps
                values.append(jnp.concatenate([one, one], axis=0).astype(BF16))
        if bt is not None:
            need = as_bf16(carry + (tile_col & 31))
            for m in range(17):
                hit = need == BF16(2 * m)
                for c in range(2):
                    bt[c * ROWS_W + 16 * m : c * ROWS_W + 16 * m + 16, lanes] = jnp.where(hit, values[c], zero)
        if sb is not None:
            need = as_bf16(carry + (tile_col & 3))
            for m in range(3):
                hit = need == BF16(2 * m)
                for c in range(2):
                    sb[c * ROWS_S + 16 * m : c * ROWS_S + 16 * m + 16, lanes] = jnp.where(hit, values[c], zero)
        if at is not None or sa is not None:
            row_taps = pick(wide(off_row, 8), tab_ref, 8)
            own_h = sub16 == wide(tile_col >> 5, 16)
            fine = (tile_col >> 2) & 7
            for b in range(2):
                spread = jnp.where(own_h, wide(row_taps[4 * b : 4 * b + 1], 16), 0.0).astype(BF16)
                row_tile = tile_row + (4 * b + g < off_row).astype(jnp.int32)
                if at is not None:
                    need = as_bf16(wide(row_tile, 16))
                    for t in range(8):
                        first = b * 128 + t * 16
                        at[first : first + 16, lanes] = jnp.where(need == BF16(t), spread, zero)
                if sa is not None:
                    need = as_bf16(wide(jnp.where(row_tile == 8, fine, -1), 16))
                    for t in range(8):
                        first = b * 128 + t * 16
                        sa[first : first + 16, lanes] = jnp.where(need == BF16(t), spread, zero)


def grid_block(vis_ref, tile_ref, off_ref, slab, g, tab_ref, scratch, main, spill):
    bt, at, sa, sb, acc, accs = scratch

    def step(i, _):
        start = pl.multiple_of(i * CHUNK, CHUNK)
        parts = (bt if main else None, at if main else None, sa if spill else None, sb if spill else None)
        build(vis_ref, tile_ref, off_ref, start, slab, g, tab_ref, parts)
        if main:
            acc[...] += dot(bt[...], at[...], NT)
        if spill:
            accs[...] += dot(sa[...], sb[...], NT)
        return 0

    lax.fori_loop(0, N_VIS // CHUNK, step, 0)


def add_spill(acc, got):
    for c in range(2):
        for b in range(2):
            for f in range(8):
                rows = pl.ds(c * ROWS_W + 32 * f, ROWS_S)
                acc[rows, b * 128 : b * 128 + 16] += got[
                    c * ROWS_S : (c + 1) * ROWS_S, b * 128 + f * 16 : b * 128 + f * 16 + 16
                ]


def row_transform(acc, d_hi, d_lo, tw, w_hi, w_lo, out_ref):
    n = ROWS_W
    p = dot3(halves(acc[...]), (d_hi[...], d_lo[...]), NN)
    real = p[:n, :256] - p[n:, 256:]
    imag = p[:n, 256:] + p[n:, :256]
    cos = jnp.concatenate([tw[0], tw[0]], axis=1)
    sin = jnp.concatenate([tw[1], tw[1]], axis=1)
    turned = (real * cos - imag * sin, real * sin + imag * cos)
    both = jnp.concatenate([jnp.concatenate([t[:16] + t[256:], t[16:256]], axis=0) for t in turned], axis=0)
    s = dot3((w_hi[...], w_lo[...]), halves(both), NN)
    for c in range(2):
        for b in range(2):
            out_ref[:, 2 * c + b, :] = s[c * 256 : (c + 1) * 256, b * 128 : (b + 1) * 128]


def fft8(x):
    def add(a, b):
        return (a[0] + b[0], a[1] + b[1])

    def sub(a, b):
        return (a[0] - b[0], a[1] - b[1])

    def by_i(a):
        return (-a[1], a[0])

    def fft4(a):
        s, d = add(a[0], a[2]), sub(a[0], a[2])
        t, e = add(a[1], a[3]), by_i(sub(a[1], a[3]))
        return [add(s, t), add(d, e), sub(s, t), sub(d, e)]

    root = np.float32(np.sqrt(0.5))
    even, odd = fft4(x[0::2]), fft4(x[1::2])
    one, three = odd[1], odd[3]
    odd[1] = (root * (one[0] - one[1]), root * (one[0] + one[1]))
    odd[2] = by_i(odd[2])
    odd[3] = (root * (-three[0] - three[1]), root * (three[0] - three[1]))
    return [add(even[k], odd[k]) for k in range(4)] + [sub(even[k], odd[k]) for k in range(4)]


def column_transform(r_ref, e_hi, e_lo, tw1, d_hi, d_lo, tw2, out_ref):
    sums = []
    for j in range(8):
        b, g = divmod(j, 4)
        x = jnp.concatenate([r_ref[pl.ds(g, 64, stride=4), 2 * c + b, :] for c in range(2)], axis=0)
        z = dot3((e_hi[...], e_lo[...]), halves(x), NN)
        real, imag = z[:128], z[128:]
        cos, sin = tw1[0], tw1[1]
        turned = jnp.concatenate([real * cos - imag * sin, real * sin + imag * cos], axis=0)
        p = dot3((d_hi[...], d_lo[...]), halves(turned), NT)
        real = p[:64, :128] - p[64:, 128:]
        imag = p[:64, 128:] + p[64:, :128]
        cos = jnp.concatenate([jnp.broadcast_to(tw2[0, 4 * j + k : 4 * j + k + 1], (16, 128)) for k in range(4)], axis=0)
        sin = jnp.concatenate([jnp.broadcast_to(tw2[1, 4 * j + k : 4 * j + k + 1], (16, 128)) for k in range(4)], axis=0)
        sums.append((real * cos - imag * sin, real * sin + imag * cos))
    for k2, pair in enumerate(fft8(sums)):
        for c in range(2):
            for k1 in range(4):
                first = 512 * k2 + 128 * k1
                out_ref[c, :, first : first + 128] = pair[c][16 * k1 : 16 * k1 + 16]


def image_kernel(*refs):
    inputs, out_ref, refs = refs[:15], refs[15], refs[16:]
    local, refs = refs[:15], refs[15:]
    own_vis, own_tiles, own_offs, kern = local[:4]
    (
        got_vis, got_tiles, got_offs, tab, bt, at, sa, sb, acc, accs, spill_out, spill_in, blocks, received,
        load_sems, send_sems, recv_sems, spill_sems, block_sems,
    ) = refs
    slab, g = lax.axis_index("rows"), lax.axis_index("grp")
    slabs, groups = lax.axis_size("rows"), lax.axis_size("grp")
    n_dev = slabs * groups
    after, before = lax.rem(slab + 1, slabs), lax.rem(slab + slabs - 1, slabs)
    low = lax.rem(g, 2)
    sibling = g + 1 - 2 * low
    across = lax.rem(g + 2, 4)
    me = slab * groups + g

    def peer(t):
        z = lax.rem(slab // 8 + lax.rem(t, 8), 8)
        x = lax.rem((slab // 2) % 4 + lax.rem(t // 8, 4), 4)
        y = lax.rem((g // 2) * 2 + slab % 2 + lax.rem(t // 32, 4), 4)
        core = lax.rem(low + t // 128, 2)
        return z * 8 + x * 2 + y % 2, (y // 2) * 2 + core

    loads = []
    for n, (source, target) in enumerate(zip(inputs, local)):
        loads.append(pltpu.make_async_copy(source, target, load_sems.at[n]))
        loads[-1].start()

    barrier = pltpu.get_barrier_semaphore()

    def greet(t, _):
        pl.semaphore_signal(barrier, inc=1, device_id=peer(t), device_id_type=MESH)
        return 0

    lax.fori_loop(1, n_dev, greet, 0)

    acc[...] = jnp.zeros_like(acc)
    accs[...] = jnp.zeros_like(accs)
    for load in loads[:4]:
        load.wait()
    build_tables(kern, g, tab)

    def send(sources, slot, to):
        copies = []
        for n, (source, target) in enumerate(zip(sources, (got_vis, got_tiles, got_offs))):
            copies.append(
                pltpu.make_async_remote_copy(
                    src_ref=source,
                    dst_ref=target.at[slot],
                    send_sem=send_sems.at[slot, n],
                    recv_sem=recv_sems.at[slot, n],
                    device_id=(slab, to),
                    device_id_type=MESH,
                )
            )
        for copy in copies:
            copy.start()
        return copies

    own = (own_vis, own_tiles, own_offs)
    held = [own] + [(got_vis.at[n], got_tiles.at[n], got_offs.at[n]) for n in range(3)]
    scratch = (bt, at, sa, sb, acc, accs)

    def block(n, main, spill):
        grid_block(*held[n], slab, g, tab, scratch, main, spill)

    block(0, True, True)
    pl.semaphore_wait(barrier, n_dev - 1)
    to_across = send(own, 1, across)
    to_sibling = send(own, 0, sibling)
    for copy in to_sibling:
        copy.wait_recv()
    block(1, True, True)
    for copy in to_across:
        copy.wait_recv()
    relayed = send(held[2], 2, sibling)
    block(2, False, True)
    for copy in relayed:
        copy.wait_recv()
    block(3, False, True)
    spill_out[...] = accs[...].T
    spill_copy = pltpu.make_async_remote_copy(
        src_ref=spill_out,
        dst_ref=spill_in,
        send_sem=spill_sems.at[0],
        recv_sem=spill_sems.at[1],
        device_id=(after, g),
        device_id_type=MESH,
    )
    spill_copy.start()
    block(2, True, False)
    block(3, True, False)
    spill_copy.wait_recv()
    add_spill(acc, spill_in)
    for load in loads[4:]:
        load.wait()
    row_transform(acc, *local[4:9], blocks)

    def block_copy(source, target, to):
        return pltpu.make_async_remote_copy(
            src_ref=blocks.at[source],
            dst_ref=received.at[target],
            send_sem=block_sems.at[0],
            recv_sem=block_sems.at[1],
            device_id=to,
            device_id_type=MESH,
        )

    def send_block(t, _):
        row, col = peer(t)
        block_copy(row * groups + col, me, (row, col)).start()
        return 0

    lax.fori_loop(1, n_dev, send_block, 0)
    received[me] = blocks[me]
    everything = block_copy(pl.ds(0, n_dev - 1), pl.ds(0, n_dev - 1), (slab, sibling))
    everything.wait_recv()
    column_transform(received, *local[9:], out_ref)
    for copy in to_sibling + to_across + relayed + [spill_copy]:
        copy.wait_send()
    everything.wait_send()


def vmem(shape, dtype):
    return pltpu.VMEM(shape, dtype)


def grid_scratch():
    return [
        vmem((16, 8, 128), F32),
        vmem((2 * ROWS_W, CHUNK), BF16),
        vmem((256, CHUNK), BF16),
        vmem((256, CHUNK), BF16),
        vmem((2 * ROWS_S, CHUNK), BF16),
        vmem((2 * ROWS_W, 256), F32),
        vmem((256, 2 * ROWS_S), F32),
        vmem((2 * ROWS_S, 256), F32),
        vmem((2 * ROWS_S, 256), F32),
    ]


def shards(visibilities, uv_tiles, kernel_offsets, kernel):
    in_hbm = pl.BlockSpec(memory_space=pltpu.HBM)
    tables = tables_v() + tables_u()
    return pl.pallas_call(
        image_kernel,
        out_shape=jax.ShapeDtypeStruct((2, 16, G), F32),
        in_specs=[in_hbm] * 15,
        out_specs=pl.BlockSpec(memory_space=pltpu.VMEM),
        scratch_shapes=[
            vmem((2, N_VIS), F32),
            vmem((2, N_VIS), jnp.int32),
            vmem((2, N_VIS), jnp.int32),
            pltpu.SMEM((8, 8), F32),
        ]
        + [vmem(t.shape, t.dtype) for t in tables]
        + [
            vmem((3, 2, N_VIS), F32),
            vmem((3, 2, N_VIS), jnp.int32),
            vmem((3, 2, N_VIS), jnp.int32),
        ]
        + grid_scratch()
        + [
            vmem((256, 4, 128), F32),
            vmem((256, 4, 128), F32),
            pltpu.SemaphoreType.DMA((15,)),
            pltpu.SemaphoreType.DMA((3, 3)),
            pltpu.SemaphoreType.DMA((3, 3)),
            pltpu.SemaphoreType.DMA((2,)),
            pltpu.SemaphoreType.DMA((2,)),
        ],
        compiler_params=pltpu.CompilerParams(
            collective_id=0, has_side_effects=True, vmem_limit_bytes=67_043_328
        ),
        name="dirty_image",
    )(visibilities, uv_tiles, kernel_offsets, kernel, *tables)


def solution(mesh):
    in_specs = (P(None, ("rows", "grp")), P(None, ("rows", "grp")), P(None, ("rows", "grp")), P())
    out_specs = P(None, ("rows", "grp"), None)
    return jax.shard_map(shards, mesh=mesh, in_specs=in_specs, out_specs=out_specs, check_vma=False)
```

```python
import functools

import jax
import jax.numpy as jnp
import numpy as np
from jax import lax
from jax.experimental import pallas as pl
from jax.experimental.pallas import tpu as pltpu
from jax.sharding import PartitionSpec as P

G = 4096
LOGICAL = pl.DeviceIdType.LOGICAL
BF16 = jnp.bfloat16
F32 = jnp.float32
CHUNK = 1024
N_VIS = 4096
ROWS_W = 272
ROWS_S = 48


def split_table(x):
    hi = x.astype(np.float32).astype(jnp.dtype(BF16))
    return hi, (x - hi.astype(np.float64)).astype(np.float32).astype(jnp.dtype(BF16))


def unit(turns):
    angle = 2.0 * np.pi * (turns % 1.0)
    return np.cos(angle), np.sin(angle)


@functools.cache
def tables_v():
    h = np.arange(16)
    er, ei = unit(h[:, None] * h[None, :] / 16)
    d = np.concatenate([np.kron(np.eye(16), er), np.kron(np.eye(16), ei)], axis=1)
    w, lane = np.arange(ROWS_W), np.arange(128)
    tr, ti = unit(w[:, None] * (lane % 16)[None, :] / 4096)
    tw = np.stack([tr, ti]).astype(np.float32) / np.float32(G)
    q = np.arange(256)
    wr, wi = unit(q[:, None] * q[None, :] / 256)
    big = np.block([[wr, -wi], [wi, wr]])
    return split_table(d) + (tw,) + split_table(big)


@functools.cache
def tables_u():
    k, s = np.arange(128), np.arange(64)
    er, ei = unit(k[:, None] * s[None, :] / 64)
    e = np.block([[er, -ei], [ei, er]])
    lane = np.arange(128)
    tr, ti = unit(k[:, None] * (lane // 16)[None, :] / 512)
    tw1 = np.stack([tr, ti]).astype(np.float32)
    row = np.arange(64)
    dr, di = unit((row // 16)[:, None] * (lane // 16)[None, :] / 4)
    same = (row % 16)[:, None] == (lane % 16)[None, :]
    d = np.concatenate([dr * same, di * same], axis=0)
    j, k1 = np.arange(8), np.arange(4)
    ar, ai = unit(j[:, None, None] * (k[None, None, :] + 128 * k1[None, :, None]) / 4096)
    tw2 = np.stack([ar.reshape(32, 128), ai.reshape(32, 128)]).astype(np.float32)
    return split_table(e) + (tw1,) + split_table(d) + (tw2,)


def halves(x):
    hi = x.astype(BF16)
    return hi, (x - hi.astype(F32)).astype(BF16)


def dot(a, b, dims):
    return lax.dot_general(a, b, (dims, ((), ())), preferred_element_type=F32)


def dot3(a, b, dims):
    return dot(a[0], b[0], dims) + (dot(a[1], b[0], dims) + dot(a[0], b[1], dims))


NN = ((1,), (0,))
NT = ((1,), (1,))


def build_tables(kern_ref, g, tab_ref):
    sub = lax.broadcasted_iota(jnp.int32, (8, 128), 0)
    for o in range(8):
        col = jnp.zeros((8, 128), F32)
        row = jnp.zeros((8, 128), F32)
        for j in range(8):
            col = jnp.where(sub == j, kern_ref[o, (j - o) % 8], col)
            row = jnp.where(sub == j, kern_ref[o, lax.rem(g + (j - o) % 8, 8)], row)
        tab_ref[o] = col
        tab_ref[8 + o] = row.astype(BF16).astype(F32)


def pick(which, tab_ref, first):
    out = jnp.zeros((8, 128), F32)
    for o in range(8):
        out = jnp.where(which == o, tab_ref[first + o], out)
    return out


def build(vis_ref, tile_ref, off_ref, start, slab, g, tab_ref, parts):
    bt, at, sa, sb = parts
    sub8 = lax.broadcasted_iota(jnp.int32, (8, 128), 0)
    sub16 = lax.broadcasted_iota(jnp.int32, (16, 128), 0)
    half = sub16 // 8
    zero = jnp.zeros((16, 128), BF16)

    def wide(x, rows):
        return jnp.broadcast_to(x, (rows, 128))

    def as_bf16(x):
        return x.astype(F32).astype(BF16)

    for q in range(CHUNK // 128):
        here = pl.ds(start + q * 128, 128)
        lanes = slice(q * 128, (q + 1) * 128)
        tile_row = tile_ref[0:1, here] - 8 * slab
        tile_col = tile_ref[1:2, here]
        off_row = off_ref[0:1, here]
        off_col = off_ref[1:2, here]
        if bt is not None or sb is not None:
            taps = pick(wide(off_col, 8), tab_ref, 0)
            wrapped = (sub8 < off_col).astype(jnp.int32)
            carry = jnp.concatenate([wrapped, wrapped], axis=0) - half
            values = []
            for c in range(2):
                one = vis_ref[c : c + 1, here] * taps
                values.append(jnp.concatenate([one, one], axis=0).astype(BF16))
        if bt is not None:
            need = as_bf16(carry + (tile_col & 31))
            for m in range(17):
                hit = need == BF16(2 * m)
                for c in range(2):
                    bt[c * ROWS_W + 16 * m : c * ROWS_W + 16 * m + 16, lanes] = jnp.where(hit, values[c], zero)
        if sb is not None:
            need = as_bf16(carry + (tile_col & 3))
            for m in range(3):
                hit = need == BF16(2 * m)
                for c in range(2):
                    sb[c * ROWS_S + 16 * m : c * ROWS_S + 16 * m + 16, lanes] = jnp.where(hit, values[c], zero)
        if at is not None or sa is not None:
            row_taps = pick(wide(off_row, 8), tab_ref, 8)
            own_h = sub16 == wide(tile_col >> 5, 16)
            fine = (tile_col >> 2) & 7
            for b in range(2):
                spread = jnp.where(own_h, wide(row_taps[4 * b : 4 * b + 1], 16), 0.0).astype(BF16)
                row_tile = tile_row + (4 * b + g < off_row).astype(jnp.int32)
                if at is not None:
                    need = as_bf16(wide(row_tile, 16))
                    for t in range(8):
                        first = b * 128 + t * 16
                        at[first : first + 16, lanes] = jnp.where(need == BF16(t), spread, zero)
                if sa is not None:
                    need = as_bf16(wide(jnp.where(row_tile == 8, fine, -1), 16))
                    for t in range(8):
                        first = b * 128 + t * 16
                        sa[first : first + 16, lanes] = jnp.where(need == BF16(t), spread, zero)


def grid_block(vis_ref, tile_ref, off_ref, slab, g, tab_ref, scratch, main, spill):
    bt, at, sa, sb, acc, accs = scratch

    def step(i, _):
        start = pl.multiple_of(i * CHUNK, CHUNK)
        parts = (bt if main else None, at if main else None, sa if spill else None, sb if spill else None)
        build(vis_ref, tile_ref, off_ref, start, slab, g, tab_ref, parts)
        if main:
            acc[...] += dot(bt[...], at[...], NT)
        if spill:
            accs[...] += dot(sa[...], sb[...], NT)
        return 0

    lax.fori_loop(0, N_VIS // CHUNK, step, 0)


def add_spill(acc, got):
    for c in range(2):
        for b in range(2):
            for f in range(8):
                rows = pl.ds(c * ROWS_W + 32 * f, ROWS_S)
                acc[rows, b * 128 : b * 128 + 16] += got[
                    c * ROWS_S : (c + 1) * ROWS_S, b * 128 + f * 16 : b * 128 + f * 16 + 16
                ]


def row_transform(acc, d_hi, d_lo, tw, w_hi, w_lo, out_ref):
    n = ROWS_W
    p = dot3(halves(acc[...]), (d_hi[...], d_lo[...]), NN)
    real = p[:n, :256] - p[n:, 256:]
    imag = p[:n, 256:] + p[n:, :256]
    cos = jnp.concatenate([tw[0], tw[0]], axis=1)
    sin = jnp.concatenate([tw[1], tw[1]], axis=1)
    turned = (real * cos - imag * sin, real * sin + imag * cos)
    both = jnp.concatenate([jnp.concatenate([t[:16] + t[256:], t[16:256]], axis=0) for t in turned], axis=0)
    s = dot3((w_hi[...], w_lo[...]), halves(both), NN)
    for c in range(2):
        for b in range(2):
            out_ref[:, 2 * c + b, :] = s[c * 256 : (c + 1) * 256, b * 128 : (b + 1) * 128]


def fft8(x):
    def add(a, b):
        return (a[0] + b[0], a[1] + b[1])

    def sub(a, b):
        return (a[0] - b[0], a[1] - b[1])

    def by_i(a):
        return (-a[1], a[0])

    def fft4(a):
        s, d = add(a[0], a[2]), sub(a[0], a[2])
        t, e = add(a[1], a[3]), by_i(sub(a[1], a[3]))
        return [add(s, t), add(d, e), sub(s, t), sub(d, e)]

    root = np.float32(np.sqrt(0.5))
    even, odd = fft4(x[0::2]), fft4(x[1::2])
    one, three = odd[1], odd[3]
    odd[1] = (root * (one[0] - one[1]), root * (one[0] + one[1]))
    odd[2] = by_i(odd[2])
    odd[3] = (root * (-three[0] - three[1]), root * (three[0] - three[1]))
    return [add(even[k], odd[k]) for k in range(4)] + [sub(even[k], odd[k]) for k in range(4)]


def column_transform(r_ref, e_hi, e_lo, tw1, d_hi, d_lo, tw2, out_ref):
    sums = []
    for j in range(8):
        b, g = divmod(j, 4)
        x = jnp.concatenate([r_ref[pl.ds(g, 64, stride=4), 2 * c + b, :] for c in range(2)], axis=0)
        z = dot3((e_hi[...], e_lo[...]), halves(x), NN)
        real, imag = z[:128], z[128:]
        cos, sin = tw1[0], tw1[1]
        turned = jnp.concatenate([real * cos - imag * sin, real * sin + imag * cos], axis=0)
        p = dot3((d_hi[...], d_lo[...]), halves(turned), NT)
        real = p[:64, :128] - p[64:, 128:]
        imag = p[:64, 128:] + p[64:, :128]
        cos = jnp.concatenate([jnp.broadcast_to(tw2[0, 4 * j + k : 4 * j + k + 1], (16, 128)) for k in range(4)], axis=0)
        sin = jnp.concatenate([jnp.broadcast_to(tw2[1, 4 * j + k : 4 * j + k + 1], (16, 128)) for k in range(4)], axis=0)
        sums.append((real * cos - imag * sin, real * sin + imag * cos))
    for k2, pair in enumerate(fft8(sums)):
        for c in range(2):
            for k1 in range(4):
                first = 512 * k2 + 128 * k1
                out_ref[c, :, first : first + 128] = pair[c][16 * k1 : 16 * k1 + 16]


def image_kernel(*refs):
    inputs, out_ref, refs = refs[:15], refs[15], refs[16:]
    local, refs = refs[:15], refs[15:]
    own_vis, own_tiles, own_offs, kern = local[:4]
    (
        got_vis, got_tiles, got_offs, tab, bt, at, sa, sb, acc, accs, spill_out, spill_in, blocks, received,
        load_sems, send_sems, recv_sems, spill_sems, block_sems, plane_sem, all_sem,
    ) = refs
    slab, g = lax.axis_index("rows"), lax.axis_index("grp")
    slabs, groups = lax.axis_size("rows"), lax.axis_size("grp")
    n_dev = slabs * groups
    after, before = lax.rem(slab + 1, slabs), lax.rem(slab + slabs - 1, slabs)
    me = slab * groups + g
    sibling, across = me ^ 1, me ^ 2
    after, before = after * groups + g, before * groups + g

    loads = []
    for n, (source, target) in enumerate(zip(inputs, local)):
        loads.append(pltpu.make_async_copy(source, target, load_sems.at[n]))
        loads[-1].start()

    barrier = pltpu.get_barrier_semaphore()

    line_x = [me ^ (8 * x) for x in range(1, 4)]
    line_z = [me ^ (32 * z) for z in range(1, 8)]
    first = [me ^ y for y in range(1, 8)] + line_x + line_z + [after, before]
    for to in first:
        pl.semaphore_signal(barrier, inc=1, device_id=to, device_id_type=LOGICAL)

    acc[...] = jnp.zeros_like(acc)
    accs[...] = jnp.zeros_like(accs)
    for load in loads[:4]:
        load.wait()
    build_tables(kern, g, tab)

    def send(sources, slot, to):
        copies = []
        for n, (source, target) in enumerate(zip(sources, (got_vis, got_tiles, got_offs))):
            copies.append(
                pltpu.make_async_remote_copy(
                    src_ref=source,
                    dst_ref=target.at[slot],
                    send_sem=send_sems.at[slot, n],
                    recv_sem=recv_sems.at[slot, n],
                    device_id=to,
                    device_id_type=LOGICAL,
                )
            )
        for copy in copies:
            copy.start()
        return copies

    own = (own_vis, own_tiles, own_offs)
    held = [own] + [(got_vis.at[n], got_tiles.at[n], got_offs.at[n]) for n in range(3)]
    scratch = (bt, at, sa, sb, acc, accs)

    def block(n, main, spill):
        grid_block(*held[n], slab, g, tab, scratch, main, spill)

    pl.semaphore_wait(barrier, len(first))
    to_across = send(own, 1, across)
    to_sibling = send(own, 0, sibling)
    for to in line_x:
        pl.semaphore_signal(plane_sem, inc=1, device_id=to, device_id_type=LOGICAL)
    block(0, True, True)
    pl.semaphore_wait(plane_sem, len(line_x))
    for to in line_z:
        pl.semaphore_signal(all_sem, inc=1, device_id=to, device_id_type=LOGICAL)
    for copy in to_sibling:
        copy.wait_recv()
    block(1, True, True)
    for copy in to_across:
        copy.wait_recv()
    relayed = send(held[2], 2, sibling)
    block(2, False, True)
    for copy in relayed:
        copy.wait_recv()
    block(3, False, True)
    spill_out[...] = accs[...].T
    spill_copy = pltpu.make_async_remote_copy(
        src_ref=spill_out,
        dst_ref=spill_in,
        send_sem=spill_sems.at[0],
        recv_sem=spill_sems.at[1],
        device_id=after,
        device_id_type=LOGICAL,
    )
    spill_copy.start()
    block(2, True, False)
    block(3, True, False)
    spill_copy.wait_recv()
    add_spill(acc, spill_in)
    for load in loads[4:]:
        load.wait()
    pl.semaphore_wait(all_sem, len(line_z))
    row_transform(acc, *local[4:9], blocks)

    def block_copy(source, target, to):
        return pltpu.make_async_remote_copy(
            src_ref=blocks.at[source],
            dst_ref=received.at[target],
            send_sem=block_sems.at[0],
            recv_sem=block_sems.at[1],
            device_id=to,
            device_id_type=LOGICAL,
        )

    def send_block(t):
        to = me ^ t
        block_copy(to, me, to).start()

    def send_blocks(low, _):
        for z in range(8):
            send_block(low ^ (32 * z))
        return 0

    for z in range(1, 8):
        send_block(32 * z)
    lax.fori_loop(1, n_dev // 8, send_blocks, 0)
    received[me] = blocks[me]
    everything = block_copy(pl.ds(0, n_dev - 1), pl.ds(0, n_dev - 1), sibling)
    everything.wait_recv()
    column_transform(received, *local[9:], out_ref)
    for copy in to_sibling + to_across + relayed + [spill_copy]:
        copy.wait_send()
    everything.wait_send()


def vmem(shape, dtype):
    return pltpu.VMEM(shape, dtype)


def grid_scratch():
    return [
        vmem((16, 8, 128), F32),
        vmem((2 * ROWS_W, CHUNK), BF16),
        vmem((256, CHUNK), BF16),
        vmem((256, CHUNK), BF16),
        vmem((2 * ROWS_S, CHUNK), BF16),
        vmem((2 * ROWS_W, 256), F32),
        vmem((256, 2 * ROWS_S), F32),
        vmem((2 * ROWS_S, 256), F32),
        vmem((2 * ROWS_S, 256), F32),
    ]


def shards(visibilities, uv_tiles, kernel_offsets, kernel):
    in_hbm = pl.BlockSpec(memory_space=pltpu.HBM)
    tables = tables_v() + tables_u()
    return pl.pallas_call(
        image_kernel,
        out_shape=jax.ShapeDtypeStruct((2, 16, G), F32),
        in_specs=[in_hbm] * 15,
        out_specs=pl.BlockSpec(memory_space=pltpu.VMEM),
        scratch_shapes=[
            vmem((2, N_VIS), F32),
            vmem((2, N_VIS), jnp.int32),
            vmem((2, N_VIS), jnp.int32),
            pltpu.SMEM((8, 8), F32),
        ]
        + [vmem(t.shape, t.dtype) for t in tables]
        + [
            vmem((3, 2, N_VIS), F32),
            vmem((3, 2, N_VIS), jnp.int32),
            vmem((3, 2, N_VIS), jnp.int32),
        ]
        + grid_scratch()
        + [
            vmem((256, 4, 128), F32),
            vmem((256, 4, 128), F32),
            pltpu.SemaphoreType.DMA((15,)),
            pltpu.SemaphoreType.DMA((3, 3)),
            pltpu.SemaphoreType.DMA((3, 3)),
            pltpu.SemaphoreType.DMA((2,)),
            pltpu.SemaphoreType.DMA((2,)),
            pltpu.SemaphoreType.REGULAR,
            pltpu.SemaphoreType.REGULAR,
        ],
        compiler_params=pltpu.CompilerParams(
            collective_id=0, has_side_effects=True, vmem_limit_bytes=67_043_328
        ),
        name="dirty_image",
    )(visibilities, uv_tiles, kernel_offsets, kernel, *tables)


def solution(mesh):
    in_specs = (P(None, ("rows", "grp")), P(None, ("rows", "grp")), P(None, ("rows", "grp")), P())
    out_specs = P(None, ("rows", "grp"), None)
    return jax.shard_map(shards, mesh=mesh, in_specs=in_specs, out_specs=out_specs, check_vma=False)
```

```python
import functools

import jax
import jax.numpy as jnp
import numpy as np
from jax import lax
from jax.experimental import pallas as pl
from jax.experimental.pallas import tpu as pltpu
from jax.sharding import PartitionSpec as P

G = 4096
LOGICAL = pl.DeviceIdType.LOGICAL
BF16 = jnp.bfloat16
F32 = jnp.float32
CHUNK = 2048
N_VIS = 4096
ROWS_W = 272
ROWS_S = 80


def split_table(x):
    hi = x.astype(np.float32).astype(jnp.dtype(BF16))
    return hi, (x - hi.astype(np.float64)).astype(np.float32).astype(jnp.dtype(BF16))


def unit(turns):
    angle = 2.0 * np.pi * (turns % 1.0)
    return np.cos(angle), np.sin(angle)


@functools.cache
def tables_v():
    h = np.arange(16)
    er, ei = unit(h[:, None] * h[None, :] / 16)
    d = np.concatenate([np.kron(np.eye(16), er), np.kron(np.eye(16), ei)], axis=1)
    w, lane = np.arange(ROWS_W), np.arange(128)
    tr, ti = unit(w[:, None] * (lane % 16)[None, :] / 4096)
    tw = np.stack([tr, ti]).astype(np.float32) / np.float32(G)
    q = np.arange(256)
    wr, wi = unit(q[:, None] * q[None, :] / 256)
    big = np.block([[wr, -wi], [wi, wr]])
    return split_table(d) + (tw,) + split_table(big)


@functools.cache
def tables_u():
    k, s = np.arange(128), np.arange(64)
    er, ei = unit(k[:, None] * s[None, :] / 64)
    e = np.block([[er, -ei], [ei, er]])
    lane = np.arange(128)
    tr, ti = unit(k[:, None] * (lane // 16)[None, :] / 512)
    tw1 = np.stack([tr, ti]).astype(np.float32)
    row = np.arange(64)
    dr, di = unit((row // 16)[:, None] * (lane // 16)[None, :] / 4)
    same = (row % 16)[:, None] == (lane % 16)[None, :]
    d = np.concatenate([dr * same, di * same], axis=0)
    j, k1 = np.arange(8), np.arange(4)
    ar, ai = unit(j[:, None, None] * (k[None, None, :] + 128 * k1[None, :, None]) / 4096)
    tw2 = np.stack([ar.reshape(32, 128), ai.reshape(32, 128)]).astype(np.float32)
    return split_table(e) + (tw1,) + split_table(d) + (tw2,)


def halves(x):
    hi = x.astype(BF16)
    return hi, (x - hi.astype(F32)).astype(BF16)


def dot(a, b, dims):
    return lax.dot_general(a, b, (dims, ((), ())), preferred_element_type=F32)


def dot3(a, b, dims):
    return dot(a[0], b[0], dims) + (dot(a[1], b[0], dims) + dot(a[0], b[1], dims))


NN = ((1,), (0,))
NT = ((1,), (1,))


def build_tables(kern_ref, g, tab_ref):
    sub = lax.broadcasted_iota(jnp.int32, (8, 128), 0)
    for o in range(8):
        col = jnp.zeros((8, 128), F32)
        row = jnp.zeros((8, 128), F32)
        for j in range(8):
            col = jnp.where(sub == j, kern_ref[o, (j - o) % 8], col)
            row = jnp.where(sub == j, kern_ref[o, lax.rem(g + (j - o) % 8, 8)], row)
        tab_ref[o] = col
        tab_ref[8 + o] = row.astype(BF16).astype(F32)


def pick(which, tab_ref, first):
    out = jnp.zeros((8, 128), F32)
    for o in range(8):
        out = jnp.where(which == o, tab_ref[first + o], out)
    return out


def build(vis_ref, tile_ref, off_ref, start, slab, g, tab_ref, parts):
    bt, at, sa, sb = parts
    sub8 = lax.broadcasted_iota(jnp.int32, (8, 128), 0)
    sub16 = lax.broadcasted_iota(jnp.int32, (16, 128), 0)
    half = sub16 // 8
    zero = jnp.zeros((16, 128), BF16)

    def wide(x, rows):
        return jnp.broadcast_to(x, (rows, 128))

    def as_bf16(x):
        return x.astype(F32).astype(BF16)

    for q in range(CHUNK // 128):
        here = pl.ds(start + q * 128, 128)
        lanes = slice(q * 128, (q + 1) * 128)
        tile_row = tile_ref[0:1, here] - 8 * slab
        tile_col = tile_ref[1:2, here]
        off_row = off_ref[0:1, here]
        off_col = off_ref[1:2, here]
        if bt is not None or sb is not None:
            taps = pick(wide(off_col, 8), tab_ref, 0)
            wrapped = (sub8 < off_col).astype(jnp.int32)
            one_of = [vis_ref[c : c + 1, here] * taps for c in range(2)]
        if bt is not None:
            need = as_bf16(jnp.concatenate([wrapped, wrapped], axis=0) - half + (tile_col & 31))
            values = [jnp.concatenate([one, one], axis=0).astype(BF16) for one in one_of]
            for m in range(17):
                hit = need == BF16(2 * m)
                for c in range(2):
                    bt[c * ROWS_W + 16 * m : c * ROWS_W + 16 * m + 16, lanes] = jnp.where(hit, values[c], zero)
        if sb is not None:
            need = as_bf16(jnp.concatenate([wrapped, wrapped], axis=0) + (tile_col & 3))
            pair = jnp.concatenate([one_of[0], one_of[1]], axis=0).astype(BF16)
            for m in range(5):
                sb[16 * m : 16 * m + 16, lanes] = jnp.where(need == BF16(m), pair, zero)
        if at is not None or sa is not None:
            row_taps = pick(wide(off_row, 8), tab_ref, 8)
            own_h = sub16 == wide(tile_col >> 5, 16)
            fine = (tile_col >> 2) & 7
            for b in range(2):
                spread = jnp.where(own_h, wide(row_taps[4 * b : 4 * b + 1], 16), 0.0).astype(BF16)
                row_tile = tile_row + (4 * b + g < off_row).astype(jnp.int32)
                if at is not None:
                    need = as_bf16(wide(row_tile, 16))
                    for t in range(8):
                        first = b * 128 + t * 16
                        at[first : first + 16, lanes] = jnp.where(need == BF16(t), spread, zero)
                if sa is not None:
                    need = as_bf16(wide(jnp.where(row_tile == 8, fine, -1), 16))
                    for t in range(8):
                        first = b * 128 + t * 16
                        sa[first : first + 16, lanes] = jnp.where(need == BF16(t), spread, zero)


def grid_blocks(slots, vis, tiles, offs, slab, g, tab_ref, scratch, main, spill):
    bt, at, sa, sb, acc, accs = scratch
    parts = ((bt, at) if main else (None, None)) + ((sa, sb) if spill else (None, None))
    per_slot = N_VIS // CHUNK

    def step(i, _):
        slot = i // per_slot
        start = pl.multiple_of(lax.rem(i, per_slot) * CHUNK, CHUNK)
        build(vis.at[slot], tiles.at[slot], offs.at[slot], start, slab, g, tab_ref, parts)
        if main:
            acc[...] += dot(bt[...], at[...], NT)
        if spill:
            accs[...] += dot(sa[...], sb[...], NT)
        return 0

    lax.fori_loop(slots[0] * per_slot, slots[1] * per_slot, step, 0)


def add_spill(acc, got):
    for c in range(2):
        for b in range(2):
            for f in range(8):
                first = c * ROWS_W + 32 * f
                for m in range(5):
                    acc[first + 8 * m : first + 8 * m + 8, b * 128 : b * 128 + 16] += got[
                        16 * m + 8 * c : 16 * m + 8 * c + 8, b * 128 + f * 16 : b * 128 + f * 16 + 16
                    ]


def row_transform(acc, d_hi, d_lo, tw, w_hi, w_lo, out_ref):
    n = ROWS_W
    p = dot3(halves(acc[...]), (d_hi[...], d_lo[...]), NN)
    real = p[:n, :256] - p[n:, 256:]
    imag = p[:n, 256:] + p[n:, :256]
    cos = jnp.concatenate([tw[0], tw[0]], axis=1)
    sin = jnp.concatenate([tw[1], tw[1]], axis=1)
    turned = (real * cos - imag * sin, real * sin + imag * cos)
    both = jnp.concatenate([jnp.concatenate([t[:16] + t[256:], t[16:256]], axis=0) for t in turned], axis=0)
    s = dot3((w_hi[...], w_lo[...]), halves(both), NN)
    for c in range(2):
        for b in range(2):
            out_ref[:, 2 * c + b, :] = s[c * 256 : (c + 1) * 256, b * 128 : (b + 1) * 128]


def fft8(x):
    def add(a, b):
        return (a[0] + b[0], a[1] + b[1])

    def sub(a, b):
        return (a[0] - b[0], a[1] - b[1])

    def by_i(a):
        return (-a[1], a[0])

    def fft4(a):
        s, d = add(a[0], a[2]), sub(a[0], a[2])
        t, e = add(a[1], a[3]), by_i(sub(a[1], a[3]))
        return [add(s, t), add(d, e), sub(s, t), sub(d, e)]

    root = np.float32(np.sqrt(0.5))
    even, odd = fft4(x[0::2]), fft4(x[1::2])
    one, three = odd[1], odd[3]
    odd[1] = (root * (one[0] - one[1]), root * (one[0] + one[1]))
    odd[2] = by_i(odd[2])
    odd[3] = (root * (-three[0] - three[1]), root * (three[0] - three[1]))
    return [add(even[k], odd[k]) for k in range(4)] + [sub(even[k], odd[k]) for k in range(4)]


def column_transform(r_ref, e_hi, e_lo, tw1, d_hi, d_lo, tw2, out_ref):
    sums = []
    for j in range(8):
        b, g = divmod(j, 4)
        x = jnp.concatenate([r_ref[pl.ds(g, 64, stride=4), 2 * c + b, :] for c in range(2)], axis=0)
        z = dot3((e_hi[...], e_lo[...]), halves(x), NN)
        real, imag = z[:128], z[128:]
        cos, sin = tw1[0], tw1[1]
        turned = jnp.concatenate([real * cos - imag * sin, real * sin + imag * cos], axis=0)
        p = dot3((d_hi[...], d_lo[...]), halves(turned), NT)
        real = p[:64, :128] - p[64:, 128:]
        imag = p[:64, 128:] + p[64:, :128]
        cos = jnp.concatenate([jnp.broadcast_to(tw2[0, 4 * j + k : 4 * j + k + 1], (16, 128)) for k in range(4)], axis=0)
        sin = jnp.concatenate([jnp.broadcast_to(tw2[1, 4 * j + k : 4 * j + k + 1], (16, 128)) for k in range(4)], axis=0)
        sums.append((real * cos - imag * sin, real * sin + imag * cos))
    for k2, pair in enumerate(fft8(sums)):
        for c in range(2):
            for k1 in range(4):
                first = 512 * k2 + 128 * k1
                out_ref[c, :, first : first + 128] = pair[c][16 * k1 : 16 * k1 + 16]


def row_kernel(*refs):
    inputs, received, refs = refs[:9], refs[9], refs[10:]
    held, local, refs = refs[:3], refs[3:9], refs[9:]
    kern, tables = local[0], local[1:]
    (
        tab, bt, at, sa, sb, acc, accs, spill_out, spill_in, blocks,
        load_sems, send_sems, recv_sems, spill_sems, block_sems, plane_sem, all_sem,
    ) = refs
    slab, g = lax.axis_index("rows"), lax.axis_index("grp")
    slabs, groups = lax.axis_size("rows"), lax.axis_size("grp")
    n_dev = slabs * groups
    after, before = lax.rem(slab + 1, slabs), lax.rem(slab + slabs - 1, slabs)
    me = slab * groups + g
    sibling, across = me ^ 1, me ^ 2
    after, before = after * groups + g, before * groups + g

    loads = []
    for n, (source, target) in enumerate(zip(inputs, [h.at[0] for h in held] + list(local))):
        loads.append(pltpu.make_async_copy(source, target, load_sems.at[n]))
        loads[-1].start()

    barrier = pltpu.get_barrier_semaphore()

    line_x = [me ^ (8 * x) for x in range(1, 4)]
    line_z = [me ^ (32 * z) for z in range(1, 8)]
    first = [me ^ y for y in range(1, 8)] + line_x + line_z + [after, before]
    for to in first:
        pl.semaphore_signal(barrier, inc=1, device_id=to, device_id_type=LOGICAL)

    acc[...] = jnp.zeros_like(acc)
    accs[...] = jnp.zeros_like(accs)
    for load in loads[:4]:
        load.wait()
    build_tables(kern, g, tab)

    def send(source, target, to):
        copies = []
        for n, ref in enumerate(held):
            copies.append(
                pltpu.make_async_remote_copy(
                    src_ref=ref.at[source],
                    dst_ref=ref.at[target],
                    send_sem=send_sems.at[target - 1, n],
                    recv_sem=recv_sems.at[target - 1, n],
                    device_id=to,
                    device_id_type=LOGICAL,
                )
            )
        for copy in copies:
            copy.start()
        return copies

    scratch = (bt, at, sa, sb, acc, accs)

    def grid(first_slot, end_slot, main, spill):
        grid_blocks((first_slot, end_slot), *held, slab, g, tab, scratch, main, spill)

    pl.semaphore_wait(barrier, len(first))
    to_across = send(0, 2, across)
    to_sibling = send(0, 1, sibling)
    for to in line_x:
        pl.semaphore_signal(plane_sem, inc=1, device_id=to, device_id_type=LOGICAL)
    grid(0, 1, True, True)
    pl.semaphore_wait(plane_sem, len(line_x))
    for to in line_z:
        pl.semaphore_signal(all_sem, inc=1, device_id=to, device_id_type=LOGICAL)
    for copy in to_sibling + to_across:
        copy.wait_recv()
    relayed = send(2, 3, sibling)
    grid(1, 3, True, True)
    for copy in relayed:
        copy.wait_recv()
    grid(3, 4, False, True)
    spill_out[...] = accs[...].T
    spill_copy = pltpu.make_async_remote_copy(
        src_ref=spill_out,
        dst_ref=spill_in,
        send_sem=spill_sems.at[0],
        recv_sem=spill_sems.at[1],
        device_id=after,
        device_id_type=LOGICAL,
    )
    spill_copy.start()
    grid(3, 4, True, False)
    spill_copy.wait_recv()
    add_spill(acc, spill_in)
    for load in loads[4:]:
        load.wait()
    pl.semaphore_wait(all_sem, len(line_z))
    row_transform(acc, *tables, blocks)

    def block_copy(source, target, to):
        return pltpu.make_async_remote_copy(
            src_ref=blocks.at[source],
            dst_ref=received.at[target],
            send_sem=block_sems.at[0],
            recv_sem=block_sems.at[1],
            device_id=to,
            device_id_type=LOGICAL,
        )

    def send_block(t):
        to = me ^ t
        block_copy(to, me, to).start()

    own_copy = pltpu.make_async_copy(blocks.at[me], received.at[me], load_sems.at[0])
    own_copy.start()

    def send_blocks(low, _):
        for z in range(8):
            send_block(low ^ (32 * z))
        return 0

    for z in range(1, 8):
        send_block(32 * z)
    lax.fori_loop(1, n_dev // 8, send_blocks, 0)
    own_copy.wait()
    everything = block_copy(pl.ds(0, n_dev - 1), pl.ds(0, n_dev - 1), sibling)
    everything.wait_recv()
    for copy in to_sibling + to_across + relayed + [spill_copy]:
        copy.wait_send()
    everything.wait_send()


def vmem(shape, dtype):
    return pltpu.VMEM(shape, dtype)


def grid_scratch():
    return [
        vmem((16, 8, 128), F32),
        vmem((2 * ROWS_W, CHUNK), BF16),
        vmem((256, CHUNK), BF16),
        vmem((256, CHUNK), BF16),
        vmem((ROWS_S, CHUNK), BF16),
        vmem((2 * ROWS_W, 256), F32),
        vmem((256, ROWS_S), F32),
        vmem((ROWS_S, 256), F32),
        vmem((ROWS_S, 256), F32),
    ]


def column_kernel(*refs):
    inputs, out_ref, local, sems = refs[:7], refs[7], refs[8:15], refs[15]
    loads = [pltpu.make_async_copy(a, b, sems.at[n]) for n, (a, b) in enumerate(zip(inputs, local))]
    for load in loads:
        load.start()
    for load in loads:
        load.wait()
    column_transform(*local, out_ref)


def shards(visibilities, uv_tiles, kernel_offsets, kernel):
    in_hbm = pl.BlockSpec(memory_space=pltpu.HBM)
    tables = tables_v()
    received = pl.pallas_call(
        row_kernel,
        out_shape=jax.ShapeDtypeStruct((256, 4, 128), F32),
        in_specs=[in_hbm] * 9,
        out_specs=in_hbm,
        scratch_shapes=[
            vmem((4, 2, N_VIS), F32),
            vmem((4, 2, N_VIS), jnp.int32),
            vmem((4, 2, N_VIS), jnp.int32),
            pltpu.SMEM((8, 8), F32),
        ]
        + [vmem(t.shape, t.dtype) for t in tables]
        + grid_scratch()
        + [
            vmem((256, 4, 128), F32),
            pltpu.SemaphoreType.DMA((9,)),
            pltpu.SemaphoreType.DMA((3, 3)),
            pltpu.SemaphoreType.DMA((3, 3)),
            pltpu.SemaphoreType.DMA((2,)),
            pltpu.SemaphoreType.DMA((2,)),
            pltpu.SemaphoreType.REGULAR,
            pltpu.SemaphoreType.REGULAR,
        ],
        compiler_params=pltpu.CompilerParams(
            collective_id=0, has_side_effects=True, vmem_limit_bytes=67_043_328
        ),
        name="row_spectra",
    )(visibilities, uv_tiles, kernel_offsets, kernel, *tables)
    tables = tables_u()
    return pl.pallas_call(
        column_kernel,
        out_shape=jax.ShapeDtypeStruct((2, 16, G), F32),
        in_specs=[in_hbm] * 7,
        out_specs=pl.BlockSpec(memory_space=pltpu.VMEM),
        scratch_shapes=[vmem((256, 4, 128), F32)]
        + [vmem(t.shape, t.dtype) for t in tables]
        + [pltpu.SemaphoreType.DMA((7,))],
        compiler_params=pltpu.CompilerParams(vmem_limit_bytes=67_043_328),
        name="column_spectra",
    )(received, *tables)


def solution(mesh):
    in_specs = (P(None, ("rows", "grp")), P(None, ("rows", "grp")), P(None, ("rows", "grp")), P())
    out_specs = P(None, ("rows", "grp"), None)
    return jax.shard_map(shards, mesh=mesh, in_specs=in_specs, out_specs=out_specs, check_vma=False)
```

```python
import functools

import jax
import jax.numpy as jnp
import numpy as np
from jax import lax
from jax.experimental import pallas as pl
from jax.experimental.pallas import tpu as pltpu
from jax.sharding import PartitionSpec as P

G = 4096
LOGICAL = pl.DeviceIdType.LOGICAL
BF16 = jnp.bfloat16
F32 = jnp.float32
CHUNK = 4096
N_VIS = 4096
ROWS_W = 272
ROWS_S = 80


def split_table(x):
    hi = x.astype(np.float32).astype(jnp.dtype(BF16))
    return hi, (x - hi.astype(np.float64)).astype(np.float32).astype(jnp.dtype(BF16))


def unit(turns):
    angle = 2.0 * np.pi * (turns % 1.0)
    return np.cos(angle), np.sin(angle)


@functools.cache
def tables_v():
    h = np.arange(16)
    er, ei = unit(h[:, None] * h[None, :] / 16)
    d = np.concatenate([np.kron(np.eye(16), er), np.kron(np.eye(16), ei)], axis=1)
    w, lane = np.arange(ROWS_W), np.arange(128)
    tr, ti = unit(w[:, None] * (lane % 16)[None, :] / 4096)
    tw = np.stack([tr, ti]).astype(np.float32) / np.float32(G)
    q = np.arange(256)
    wr, wi = unit(q[:, None] * q[None, :] / 256)
    big = np.block([[wr, -wi], [wi, wr]])
    return split_table(d) + (tw,) + split_table(big)


@functools.cache
def tables_u():
    k, s = np.arange(128), np.arange(64)
    er, ei = unit(k[:, None] * s[None, :] / 64)
    e = np.block([[er, -ei], [ei, er]])
    lane = np.arange(128)
    tr, ti = unit(k[:, None] * (lane // 16)[None, :] / 512)
    tw1 = np.stack([tr, ti]).astype(np.float32)
    row = np.arange(64)
    dr, di = unit((row // 16)[:, None] * (lane // 16)[None, :] / 4)
    same = (row % 16)[:, None] == (lane % 16)[None, :]
    d = np.concatenate([dr * same, di * same], axis=0)
    j, k1 = np.arange(8), np.arange(4)
    ar, ai = unit(j[:, None, None] * (k[None, None, :] + 128 * k1[None, :, None]) / 4096)
    tw2 = np.stack([ar.reshape(32, 128), ai.reshape(32, 128)]).astype(np.float32)
    return split_table(e) + (tw1,) + split_table(d) + (tw2,)


def halves(x):
    hi = x.astype(BF16)
    return hi, (x - hi.astype(F32)).astype(BF16)


def dot(a, b, dims):
    return lax.dot_general(a, b, (dims, ((), ())), preferred_element_type=F32)


def dot3(a, b, dims):
    return dot(a[0], b[0], dims) + (dot(a[1], b[0], dims) + dot(a[0], b[1], dims))


def dot2(table, x, dims):
    x = x.astype(BF16)
    return dot(table[0], x, dims) + dot(table[1], x, dims)


NN = ((1,), (0,))
NT = ((1,), (1,))


def build_tables(kern_ref, g, tab_ref):
    sub = lax.broadcasted_iota(jnp.int32, (8, 128), 0)
    for o in range(8):
        col = jnp.zeros((8, 128), F32)
        row = jnp.zeros((8, 128), F32)
        for j in range(8):
            col = jnp.where(sub == j, kern_ref[o, (j - o) % 8], col)
            row = jnp.where(sub == j, kern_ref[o, lax.rem(g + (j - o) % 8, 8)], row)
        tab_ref[o] = col
        tab_ref[8 + o] = row.astype(BF16).astype(F32)


def pick(which, tab_ref, first):
    out = jnp.zeros((8, 128), F32)
    for o in range(8):
        out = jnp.where(which == o, tab_ref[first + o], out)
    return out


def build(vis_ref, tile_ref, off_ref, start, slab, g, tab_ref, parts):
    bt, at, sa, sb = parts
    sub8 = lax.broadcasted_iota(jnp.int32, (8, 128), 0)
    sub16 = lax.broadcasted_iota(jnp.int32, (16, 128), 0)
    half = sub16 // 8
    zero = jnp.zeros((16, 128), BF16)

    def wide(x, rows):
        return jnp.broadcast_to(x, (rows, 128))

    def as_bf16(x):
        return x.astype(F32).astype(BF16)

    for q in range(CHUNK // 128):
        here = pl.ds(start + q * 128, 128)
        lanes = slice(q * 128, (q + 1) * 128)
        tile_row = tile_ref[0:1, here] - 8 * slab
        tile_col = tile_ref[1:2, here]
        off_row = off_ref[0:1, here]
        off_col = off_ref[1:2, here]
        if bt is not None or sb is not None:
            taps = pick(wide(off_col, 8), tab_ref, 0)
            wrapped = (sub8 < off_col).astype(jnp.int32)
            one_of = [vis_ref[c : c + 1, here] * taps for c in range(2)]
        if bt is not None:
            need = as_bf16(jnp.concatenate([wrapped, wrapped], axis=0) - half + (tile_col & 31))
            values = [jnp.concatenate([one, one], axis=0).astype(BF16) for one in one_of]
            for m in range(17):
                hit = need == BF16(2 * m)
                for c in range(2):
                    bt[c * ROWS_W + 16 * m : c * ROWS_W + 16 * m + 16, lanes] = jnp.where(hit, values[c], zero)
        if sb is not None:
            need = as_bf16(jnp.concatenate([wrapped, wrapped], axis=0) + (tile_col & 3))
            pair = jnp.concatenate([one_of[0], one_of[1]], axis=0).astype(BF16)
            for m in range(5):
                sb[16 * m : 16 * m + 16, lanes] = jnp.where(need == BF16(m), pair, zero)
        if at is not None or sa is not None:
            row_taps = pick(wide(off_row, 8), tab_ref, 8)
            own_h = sub16 == wide(tile_col >> 5, 16)
            fine = (tile_col >> 2) & 7
            for b in range(2):
                spread = jnp.where(own_h, wide(row_taps[4 * b : 4 * b + 1], 16), 0.0).astype(BF16)
                row_tile = tile_row + (4 * b + g < off_row).astype(jnp.int32)
                if at is not None:
                    need = as_bf16(wide(row_tile, 16))
                    for t in range(8):
                        first = b * 128 + t * 16
                        at[first : first + 16, lanes] = jnp.where(need == BF16(t), spread, zero)
                if sa is not None:
                    need = as_bf16(wide(jnp.where(row_tile == 8, fine, -1), 16))
                    for t in range(8):
                        first = b * 128 + t * 16
                        sa[first : first + 16, lanes] = jnp.where(need == BF16(t), spread, zero)


def grid_blocks(slots, vis, tiles, offs, slab, g, tab_ref, scratch, main, spill):
    bt, at, sa, sb, acc, accs = scratch
    parts = ((bt, at) if main else (None, None)) + ((sa, sb) if spill else (None, None))
    per_slot = N_VIS // CHUNK

    def step(i, _):
        slot = i // per_slot
        start = pl.multiple_of(lax.rem(i, per_slot) * CHUNK, CHUNK)
        build(vis.at[slot], tiles.at[slot], offs.at[slot], start, slab, g, tab_ref, parts)
        if main:
            acc[...] += dot(bt[...], at[...], NT)
        if spill:
            accs[...] += dot(sa[...], sb[...], NT)
        return 0

    lax.fori_loop(slots[0] * per_slot, slots[1] * per_slot, step, 0)


def add_spill(acc, got):
    for c in range(2):
        for b in range(2):
            for f in range(8):
                first = c * ROWS_W + 32 * f
                for m in range(5):
                    acc[first + 8 * m : first + 8 * m + 8, b * 128 : b * 128 + 16] += got[
                        16 * m + 8 * c : 16 * m + 8 * c + 8, b * 128 + f * 16 : b * 128 + f * 16 + 16
                    ]


def row_transform(acc, d_hi, d_lo, tw, w_hi, w_lo, out_ref):
    n = ROWS_W
    p = dot3(halves(acc[...]), (d_hi[...], d_lo[...]), NN)
    real = p[:n, :256] - p[n:, 256:]
    imag = p[:n, 256:] + p[n:, :256]
    cos = jnp.concatenate([tw[0], tw[0]], axis=1)
    sin = jnp.concatenate([tw[1], tw[1]], axis=1)
    turned = (real * cos - imag * sin, real * sin + imag * cos)
    both = jnp.concatenate([jnp.concatenate([t[:16] + t[256:], t[16:256]], axis=0) for t in turned], axis=0)
    s = dot2((w_hi[...], w_lo[...]), both, NN)
    for c in range(2):
        for b in range(2):
            out_ref[:, 2 * c + b, :] = s[c * 256 : (c + 1) * 256, b * 128 : (b + 1) * 128]


def fft8(x):
    def add(a, b):
        return (a[0] + b[0], a[1] + b[1])

    def sub(a, b):
        return (a[0] - b[0], a[1] - b[1])

    def by_i(a):
        return (-a[1], a[0])

    def fft4(a):
        s, d = add(a[0], a[2]), sub(a[0], a[2])
        t, e = add(a[1], a[3]), by_i(sub(a[1], a[3]))
        return [add(s, t), add(d, e), sub(s, t), sub(d, e)]

    root = np.float32(np.sqrt(0.5))
    even, odd = fft4(x[0::2]), fft4(x[1::2])
    one, three = odd[1], odd[3]
    odd[1] = (root * (one[0] - one[1]), root * (one[0] + one[1]))
    odd[2] = by_i(odd[2])
    odd[3] = (root * (-three[0] - three[1]), root * (three[0] - three[1]))
    return [add(even[k], odd[k]) for k in range(4)] + [sub(even[k], odd[k]) for k in range(4)]


def column_transform(r_ref, e_hi, e_lo, tw1, d_hi, d_lo, tw2, out_ref):
    def rows_of(j):
        b, g = divmod(j, 4)
        return jnp.concatenate([r_ref[pl.ds(g, 64, stride=4), 2 * c + b, :] for c in range(2)], axis=0)

    x = jnp.concatenate([rows_of(j) for j in range(8)], axis=1)
    z = dot2((e_hi[...], e_lo[...]), x, NN)
    cos, sin = tw1[0], tw1[1]
    turned = []
    for j in range(8):
        real, imag = z[:128, 128 * j : 128 * j + 128], z[128:, 128 * j : 128 * j + 128]
        turned += [real * cos - imag * sin, real * sin + imag * cos]
    p = dot2((d_hi[...], d_lo[...]), jnp.concatenate(turned, axis=0), NT)
    sums = []
    for j in range(8):
        first, second = p[:, 256 * j : 256 * j + 128], p[:, 256 * j + 128 : 256 * j + 256]
        real = first[:64] - second[64:]
        imag = second[:64] + first[64:]
        cos = jnp.concatenate([jnp.broadcast_to(tw2[0, 4 * j + k : 4 * j + k + 1], (16, 128)) for k in range(4)], axis=0)
        sin = jnp.concatenate([jnp.broadcast_to(tw2[1, 4 * j + k : 4 * j + k + 1], (16, 128)) for k in range(4)], axis=0)
        sums.append((real * cos - imag * sin, real * sin + imag * cos))
    for k2, pair in enumerate(fft8(sums)):
        for c in range(2):
            for k1 in range(4):
                first = 512 * k2 + 128 * k1
                out_ref[c, :, first : first + 128] = pair[c][16 * k1 : 16 * k1 + 16]


def row_kernel(*refs):
    inputs, received, refs = refs[:9], refs[9], refs[10:]
    held, local, refs = refs[:3], refs[3:9], refs[9:]
    kern, tables = local[0], local[1:]
    (
        tab, bt, at, sa, sb, acc, accs, spill_out, spill_in, blocks,
        load_sems, send_sems, recv_sems, spill_sems, block_sems, plane_sem, all_sem,
    ) = refs
    slab, g = lax.axis_index("rows"), lax.axis_index("grp")
    slabs, groups = lax.axis_size("rows"), lax.axis_size("grp")
    n_dev = slabs * groups
    after, before = lax.rem(slab + 1, slabs), lax.rem(slab + slabs - 1, slabs)
    me = slab * groups + g
    sibling, across = me ^ 1, me ^ 2
    after, before = after * groups + g, before * groups + g

    loads = []
    for n, (source, target) in enumerate(zip(inputs, [h.at[0] for h in held] + list(local))):
        loads.append(pltpu.make_async_copy(source, target, load_sems.at[n]))
        loads[-1].start()

    barrier = pltpu.get_barrier_semaphore()

    line_x = [me ^ (8 * x) for x in range(1, 4)]
    line_z = [me ^ (32 * z) for z in range(1, 8)]
    first = [me ^ y for y in range(1, 8)] + line_x + line_z + [after, before]
    for to in first:
        pl.semaphore_signal(barrier, inc=1, device_id=to, device_id_type=LOGICAL)

    acc[...] = jnp.zeros_like(acc)
    accs[...] = jnp.zeros_like(accs)
    for load in loads[:4]:
        load.wait()
    build_tables(kern, g, tab)

    def send(source, target, to):
        copies = []
        for n, ref in enumerate(held):
            copies.append(
                pltpu.make_async_remote_copy(
                    src_ref=ref.at[source],
                    dst_ref=ref.at[target],
                    send_sem=send_sems.at[target - 1, n],
                    recv_sem=recv_sems.at[target - 1, n],
                    device_id=to,
                    device_id_type=LOGICAL,
                )
            )
        for copy in copies:
            copy.start()
        return copies

    scratch = (bt, at, sa, sb, acc, accs)

    def grid(first_slot, end_slot, main, spill):
        grid_blocks((first_slot, end_slot), *held, slab, g, tab, scratch, main, spill)

    pl.semaphore_wait(barrier, len(first))
    to_across = send(0, 2, across)
    to_sibling = send(0, 1, sibling)
    for to in line_x:
        pl.semaphore_signal(plane_sem, inc=1, device_id=to, device_id_type=LOGICAL)
    grid(0, 1, True, True)
    pl.semaphore_wait(plane_sem, len(line_x))
    for to in line_z:
        pl.semaphore_signal(all_sem, inc=1, device_id=to, device_id_type=LOGICAL)
    for copy in to_sibling + to_across:
        copy.wait_recv()
    relayed = send(2, 3, sibling)
    grid(1, 3, True, True)
    for copy in relayed:
        copy.wait_recv()
    grid(3, 4, False, True)
    spill_out[...] = accs[...].T
    spill_copy = pltpu.make_async_remote_copy(
        src_ref=spill_out,
        dst_ref=spill_in,
        send_sem=spill_sems.at[0],
        recv_sem=spill_sems.at[1],
        device_id=after,
        device_id_type=LOGICAL,
    )
    spill_copy.start()
    grid(3, 4, True, False)
    spill_copy.wait_recv()
    add_spill(acc, spill_in)
    for load in loads[4:]:
        load.wait()
    pl.semaphore_wait(all_sem, len(line_z))
    row_transform(acc, *tables, blocks)

    def block_copy(source, target, to):
        return pltpu.make_async_remote_copy(
            src_ref=blocks.at[source],
            dst_ref=received.at[target],
            send_sem=block_sems.at[0],
            recv_sem=block_sems.at[1],
            device_id=to,
            device_id_type=LOGICAL,
        )

    def send_block(t):
        to = me ^ t
        block_copy(to, me, to).start()

    own_copy = pltpu.make_async_copy(blocks.at[me], received.at[me], load_sems.at[0])
    own_copy.start()

    def send_blocks(low, _):
        for z in (4, 3, 5, 2, 6, 1, 7, 0):
            send_block(low ^ (32 * z))
        return 0

    for z in range(1, 8):
        send_block(32 * z)
    lax.fori_loop(1, n_dev // 8, send_blocks, 0)
    own_copy.wait()
    everything = block_copy(pl.ds(0, n_dev - 1), pl.ds(0, n_dev - 1), sibling)
    everything.wait_recv()
    for copy in to_sibling + to_across + relayed + [spill_copy]:
        copy.wait_send()
    everything.wait_send()


def vmem(shape, dtype):
    return pltpu.VMEM(shape, dtype)


def grid_scratch():
    return [
        vmem((16, 8, 128), F32),
        vmem((2 * ROWS_W, CHUNK), BF16),
        vmem((256, CHUNK), BF16),
        vmem((256, CHUNK), BF16),
        vmem((ROWS_S, CHUNK), BF16),
        vmem((2 * ROWS_W, 256), F32),
        vmem((256, ROWS_S), F32),
        vmem((ROWS_S, 256), F32),
        vmem((ROWS_S, 256), F32),
    ]


def column_kernel(*refs):
    inputs, out_ref, local, sems = refs[:7], refs[7], refs[8:15], refs[15]
    loads = [pltpu.make_async_copy(a, b, sems.at[n]) for n, (a, b) in enumerate(zip(inputs, local))]
    for load in loads:
        load.start()
    for load in loads:
        load.wait()
    column_transform(*local, out_ref)


def shards(visibilities, uv_tiles, kernel_offsets, kernel):
    in_hbm = pl.BlockSpec(memory_space=pltpu.HBM)
    tables = tables_v()
    received = pl.pallas_call(
        row_kernel,
        out_shape=jax.ShapeDtypeStruct((256, 4, 128), F32),
        in_specs=[in_hbm] * 9,
        out_specs=in_hbm,
        scratch_shapes=[
            vmem((4, 2, N_VIS), F32),
            vmem((4, 2, N_VIS), jnp.int32),
            vmem((4, 2, N_VIS), jnp.int32),
            pltpu.SMEM((8, 8), F32),
        ]
        + [vmem(t.shape, t.dtype) for t in tables]
        + grid_scratch()
        + [
            vmem((256, 4, 128), F32),
            pltpu.SemaphoreType.DMA((9,)),
            pltpu.SemaphoreType.DMA((3, 3)),
            pltpu.SemaphoreType.DMA((3, 3)),
            pltpu.SemaphoreType.DMA((2,)),
            pltpu.SemaphoreType.DMA((2,)),
            pltpu.SemaphoreType.REGULAR,
            pltpu.SemaphoreType.REGULAR,
        ],
        compiler_params=pltpu.CompilerParams(
            collective_id=0, has_side_effects=True, vmem_limit_bytes=67_043_328
        ),
        name="row_spectra",
    )(visibilities, uv_tiles, kernel_offsets, kernel, *tables)
    tables = tables_u()
    return pl.pallas_call(
        column_kernel,
        out_shape=jax.ShapeDtypeStruct((2, 16, G), F32),
        in_specs=[in_hbm] * 7,
        out_specs=pl.BlockSpec(memory_space=pltpu.VMEM),
        scratch_shapes=[vmem((256, 4, 128), F32)]
        + [vmem(t.shape, t.dtype) for t in tables]
        + [pltpu.SemaphoreType.DMA((7,))],
        compiler_params=pltpu.CompilerParams(vmem_limit_bytes=67_043_328),
        name="column_spectra",
    )(received, *tables)


def solution(mesh):
    in_specs = (P(None, ("rows", "grp")), P(None, ("rows", "grp")), P(None, ("rows", "grp")), P())
    out_specs = P(None, ("rows", "grp"), None)
    return jax.shard_map(shards, mesh=mesh, in_specs=in_specs, out_specs=out_specs, check_vma=False)
```
